1024 devices in a mesh: gx: 32 (over x, y, core), gy: 8 (over z_lo), gz: 4 (over z_hi).
Axes of the slice: x: 4, y: 4, z: 32 (z_hi: 4, z_lo: 8; z = z_hi * 8 + z_lo), core: 2. Of those that a mesh axis runs over, the one named last changes fastest.
Arguments:
- gas_pos: float32 [3, 32, 8, 4, 2048], P(None, 'gx', 'gy', 'gz'), may hold values from 0 to 1
- gas_mass: float32 [32, 8, 4, 2048], P('gx', 'gy', 'gz'), may hold values from 0.2 to 5
- source_pos: float32 [3, 32, 8, 4, 2048], P(None, 'gx', 'gy', 'gz'), may hold values from 0 to 1
- source_radius: float32 [32, 8, 4, 2048], P('gx', 'gy', 'gz'), may hold values from 0.25 to 1
- source_yield: float32 [2, 32, 8, 4, 2048], P(None, 'gx', 'gy', 'gz'), may hold values from 1 to 30
- source_momentum: float32 [3, 32, 8, 4, 2048], P(None, 'gx', 'gy', 'gz'), may hold values from -180 to 180
- source_tiles: int32 [32, 8, 4, 16, 8], P('gx', 'gy', 'gz'), may hold values from 0 to 431, as said below
- source_count: int32 [32, 8, 4], P('gx', 'gy', 'gz'), may hold values from 1 to 2048, as said below
Outputs:
- gas_gain: float32 [5, 32, 8, 4, 2048], P(None, 'gx', 'gy', 'gz')
The draws below stay inside these ranges and needn't reach their ends.
Inputs may be any that keep to these rules, and one draw needn't show every extreme that they name: `source_tiles`: the 8 tiles of one block lie one in each of the 8 domains around one corner of the block's domain (that domain among them), in increasing order. Over all blocks of one domain, at most 8 distinct listed tiles lie in any one neighbouring slot. `source_count`: some domain holds 2048 live sources in every draw.
All inputs are finite; a program needn't handle non-finite values.
Results may differ from the reference program's by a relative error of at most 0.0003.
Values sent between devices are 32-bit elements; how exact they have to be, the bound alone decides.
No kernel may reach another device: no remote copies, remote signals or barrier semaphores. Data moves between devices by JAX's collectives and lax.ppermute only.
A program may use at most 32 MiB of HBM per device.

```python
import math
import jax
import jax.numpy as jnp
from jax import lax

GAS = 2048
SRC_BLOCKS = 16
TILES_LISTED = 8
GAS_TILES = 16
SOURCES = 2048
DOM_X = 32
DOM_Y = 8
DOM_Z = 4


def feedback_layout(key):
    base = jax.random.fold_in(key, 2024)
    streams = jax.random.split(base, 6)
    domains = DOM_X * DOM_Y * DOM_Z
    capacity = GAS_TILES // 2
    dom_ids = jnp.arange(domains, dtype=jnp.int32)
    counts = jax.random.randint(streams[0], (domains,), 1, SOURCES + 1)
    chosen = jax.random.randint(streams[1], (), 0, domains)
    counts = jnp.where(dom_ids == chosen, SOURCES, counts).astype(jnp.int32)
    scores = jax.random.randint(streams[2], (domains, 27, GAS_TILES), 0, 262144)
    scores = scores * GAS_TILES + jnp.arange(GAS_TILES, dtype=jnp.int32)[None, None, :]
    candidates = lax.top_k(scores, capacity)[1].astype(jnp.int32)
    corners = jax.random.randint(streams[3], (domains, SRC_BLOCKS), 0, 8)
    forced = jax.random.randint(streams[4], (), 0, 8)
    block_ids = jnp.arange(SRC_BLOCKS, dtype=jnp.int32)
    pinned = (dom_ids[:, None] == chosen) & (block_ids[None, :] < capacity)
    corners = jnp.where(pinned, forced, corners).astype(jnp.int32)
    rotate = jax.random.randint(streams[5], (domains, 27), 0, capacity)
    octant = jnp.arange(8, dtype=jnp.int32)
    sign_x = 2 * (corners // 4) - 1
    sign_y = 2 * (corners // 2 % 2) - 1
    sign_z = 2 * (corners % 2) - 1
    slots = 9 * (sign_x[:, :, None] * (octant // 4)[None, None, :] + 1)
    slots = slots + 3 * (sign_y[:, :, None] * (octant // 2 % 2)[None, None, :] + 1)
    slots = slots + (sign_z[:, :, None] * (octant % 2)[None, None, :] + 1)
    slot_flat = slots.reshape(domains, SRC_BLOCKS * 8)
    turned = jnp.take_along_axis(rotate, slot_flat, axis=1).reshape(domains, SRC_BLOCKS, 8)
    member = (block_ids[None, :, None] + turned) % capacity
    where_flat = (slots * capacity + member).reshape(domains, SRC_BLOCKS * 8)
    tiles = jnp.take_along_axis(candidates.reshape(domains, 27 * capacity), where_flat, axis=1)
    listed = slots * GAS_TILES + tiles.reshape(domains, SRC_BLOCKS, 8)
    listed = jnp.sort(listed, axis=-1).astype(jnp.int32)
    return (listed.reshape(DOM_X, DOM_Y, DOM_Z, SRC_BLOCKS, 8), counts.reshape(DOM_X, DOM_Y, DOM_Z))


def draw_source_tiles(key, part):
    return feedback_layout(key)[0]


def draw_source_count(key, part):
    return feedback_layout(key)[1]


def level_of(own_key, shape, shards, least, high):
    factor_of, own = 1.0, jax.random.fold_in(own_key, 6)
    for axis_at, shards_of in shards:
        draws = jnp.exp(jax.random.uniform(jax.random.fold_in(own, axis_at), (shards_of,), jnp.float32, least / len(shards), high / len(shards)))
        factor_of = factor_of * jnp.repeat(draws, shape[axis_at] // shards_of).reshape([-1 if axis == axis_at else 1 for axis in range(len(shape))])
    return factor_of


def normal_values(rng, extent, scale, bound, cuts=(), kind=jnp.bfloat16):
    level = level_of(rng, extent, cuts, -0.22, 0.18) if cuts else 1.0
    drawn = jax.random.normal(rng, extent, jnp.float32) * scale * level
    return jnp.minimum(jnp.maximum(drawn, -bound), bound).astype(kind)


def setup_inputs(seed: int = 0) -> dict:
    key_of = jax.random.split(jax.random.key(seed), 9)
    gas_pos = jnp.clip(1.0 * jax.random.uniform(key_of[0], (3, DOM_X, DOM_Y, DOM_Z, GAS), jnp.float32) ** level_of(key_of[0], (3, DOM_X, DOM_Y, DOM_Z, GAS), ((1, 32), (2, 8), (3, 4)), -0.2, 0.2), 0.0, 1.0)
    gas_mass = jnp.clip(jnp.exp(math.log(5.0) - 3.218876 * jax.random.uniform(key_of[1], (DOM_X, DOM_Y, DOM_Z, GAS), jnp.float32) ** level_of(key_of[1], (DOM_X, DOM_Y, DOM_Z, GAS), ((0, 32), (1, 8), (2, 4)), -0.2, 0.2)), 0.2, 5.0)
    source_pos = jnp.clip(1.0 * jax.random.uniform(key_of[2], (3, DOM_X, DOM_Y, DOM_Z, SOURCES), jnp.float32) ** level_of(key_of[2], (3, DOM_X, DOM_Y, DOM_Z, SOURCES), ((1, 32), (2, 8), (3, 4)), -0.2, 0.2), 0.0, 1.0)
    source_radius = jnp.clip(jnp.exp(math.log(1.0) - 1.3862944 * jax.random.uniform(key_of[3], (DOM_X, DOM_Y, DOM_Z, SOURCES), jnp.float32) ** level_of(key_of[3], (DOM_X, DOM_Y, DOM_Z, SOURCES), ((0, 32), (1, 8), (2, 4)), -0.2, 0.2)), 0.25, 1.0)
    source_yield = jnp.clip(jnp.exp(math.log(30.0) - 3.4011974 * jax.random.uniform(key_of[4], (2, DOM_X, DOM_Y, DOM_Z, SOURCES), jnp.float32) ** level_of(key_of[4], (2, DOM_X, DOM_Y, DOM_Z, SOURCES), ((1, 32), (2, 8), (3, 4)), -0.2, 0.2)), 1.0, 30.0)
    source_momentum = normal_values(key_of[5], (3, DOM_X, DOM_Y, DOM_Z, SOURCES), 30.0, 180.0, ((1, 32), (2, 8), (3, 4)), jnp.float32)
    source_tiles = draw_source_tiles(jax.random.fold_in(key_of[8], 71), 0)
    source_count = draw_source_count(jax.random.fold_in(key_of[8], 71), 0)
    return dict(gas_pos=gas_pos, gas_mass=gas_mass, source_pos=source_pos, source_radius=source_radius, source_yield=source_yield, source_momentum=source_momentum, source_tiles=source_tiles, source_count=source_count)


def block_deposit(near, tile_ids, source_xyz, inv_square, load, live, tiles_each):
    picked = jnp.take(near, tile_ids, axis=1)
    slot = tile_ids // tiles_each
    shifts = jnp.stack([slot // 9 - 1, (slot // 3) % 3 - 1, slot % 3 - 1]).astype(near.dtype)
    gas_xyz = (picked[0:3] + shifts[:, :, None]).reshape(3, -1)
    masses = picked[3].reshape(-1)
    dist_sq = jnp.square(gas_xyz[0][None, :] - source_xyz[0][:, None])
    dist_sq = dist_sq + jnp.square(gas_xyz[1][None, :] - source_xyz[1][:, None])
    dist_sq = dist_sq + jnp.square(gas_xyz[2][None, :] - source_xyz[2][:, None])
    weight = masses[None, :] / jnp.square(1.0 + dist_sq * inv_square[:, None])
    norm_sum = jnp.sum(weight, axis=1)
    coeffs = load * (live / norm_sum)[None, :]
    moved = jnp.dot(coeffs, weight, precision=lax.Precision.HIGHEST, preferred_element_type=jnp.float32)
    return moved.reshape(load.shape[0], tile_ids.shape[0], 128)


def reference(gas_pos, gas_mass, source_pos, source_radius, source_yield, source_momentum, source_tiles, source_count):
    gas_all = jnp.concatenate([gas_pos, gas_mass[None]], axis=0)
    load_all = jnp.concatenate([source_yield[0:1], source_momentum, source_yield[1:2]], axis=0)
    inv_all = (1.0 / jnp.square(source_radius))[None]
    zero = jnp.zeros((), jnp.int32)
    gain_init = jnp.zeros((5, DOM_X, DOM_Y, DOM_Z, GAS), jnp.float32)

    def per_device(gain, flat):
        ix = (flat // (DOM_Y * DOM_Z)).astype(jnp.int32)
        iy = ((flat // DOM_Z) % DOM_Y).astype(jnp.int32)
        iz = (flat % DOM_Z).astype(jnp.int32)
        starts = []
        for slot in range(27):
            sx = ((ix + slot // 9 - 1) % DOM_X).astype(jnp.int32)
            sy = ((iy + (slot // 3) % 3 - 1) % DOM_Y).astype(jnp.int32)
            sz = ((iz + slot % 3 - 1) % DOM_Z).astype(jnp.int32)
            starts.append((zero, sx, sy, sz, zero))
        pieces = [lax.dynamic_slice(gas_all, start, (4, 1, 1, 1, GAS)).reshape(4, GAS) for start in starts]
        near = jnp.stack(pieces, axis=1).reshape(4, 27 * GAS_TILES, 128)

        def own_rows(array):
            rows = lax.dynamic_slice(array, (zero, ix, iy, iz, zero), (array.shape[0], 1, 1, 1, SOURCES))
            return rows.reshape(array.shape[0], SRC_BLOCKS, 128)

        source_xyz = own_rows(source_pos)
        loads = own_rows(load_all)
        inv_sq = own_rows(inv_all)[0]
        tile_table = lax.dynamic_slice(source_tiles, (ix, iy, iz, zero, zero), (1, 1, 1, SRC_BLOCKS, TILES_LISTED)).reshape(SRC_BLOCKS, TILES_LISTED)
        live_count = lax.dynamic_slice(source_count, (ix, iy, iz), (1, 1, 1)).reshape(())
        used_blocks = ((live_count + 127) // 128).astype(jnp.int32)

        def add_block(block_idx, acc):
            live = (block_idx * 128 + jnp.arange(128, dtype=jnp.int32) < live_count).astype(gas_all.dtype)
            ids = lax.dynamic_index_in_dim(tile_table, block_idx, 0, keepdims=False)
            xyz_rows = lax.dynamic_index_in_dim(source_xyz, block_idx, 1, keepdims=False)
            inv_rows = lax.dynamic_index_in_dim(inv_sq, block_idx, 0, keepdims=False)
            load_rows = lax.dynamic_index_in_dim(loads, block_idx, 1, keepdims=False)
            moved = block_deposit(near, ids, xyz_rows, inv_rows, load_rows, live, GAS_TILES)
            return acc.at[:, ids].add(moved)

        acc_init = jnp.zeros((5, 27 * GAS_TILES, 128), jnp.float32)
        acc = lax.fori_loop(zero, used_blocks, add_block, acc_init)
        spread = acc.reshape(5, 27, GAS)
        for slot in range(27):
            current = lax.dynamic_slice(gain, starts[slot], (5, 1, 1, 1, GAS))
            gain = lax.dynamic_update_slice(gain, current + spread[:, slot].reshape(5, 1, 1, 1, GAS), starts[slot])
        return gain, None

    gain, unused_all = lax.scan(per_device, gain_init, jnp.arange(DOM_X * DOM_Y * DOM_Z, dtype=jnp.int32))
    return gain / gas_mass[None]
```

```python
import math

import jax
import jax.numpy as jnp
from jax import lax
from jax.sharding import PartitionSpec as P


def padded_2(shard, sides, width):
    for axis, dim in sides:
        count, length = (lax.axis_size(axis), shard.shape[dim])
        up = [(i, (i + 1) % count) for i in range(count)]
        down = [(j, i) for i, j in up]
        last = lax.slice_in_dim(shard, length - width, length, axis=dim)
        leading = lax.slice_in_dim(shard, 0, width, axis=dim)
        before = lax.ppermute(last, axis, up)
        after = lax.ppermute(leading, axis, down)
        shard = jnp.concatenate([before, shard, after], axis=dim)
    return shard


def folded(slots, axis):
    count = lax.axis_size(axis)
    up = [(i, (i + 1) % count) for i in range(count)]
    down = [(j, i) for i, j in up]
    before = lax.ppermute(slots[:, 2], axis, up)
    after = lax.ppermute(slots[:, 0], axis, down)
    return slots[:, 1] + before + after


def group_deposit(near, tile_ids, source_xyz, inv_square, load, live, tiles_each):
    picked = jnp.take(near, tile_ids, axis=1)
    width = tile_ids.shape[0]
    slot = tile_ids // tiles_each
    shifts = jnp.stack([slot // 9 - 1, slot // 3 % 3 - 1, slot % 3 - 1]).astype(near.dtype)
    gas_xyz = (picked[0:3] + shifts[:, :, :, None]).reshape(3, width, -1)
    masses = picked[3].reshape(width, -1)
    dist_sq = jnp.square(gas_xyz[0][:, None, :] - source_xyz[0][:, :, None])
    dist_sq = dist_sq + jnp.square(gas_xyz[1][:, None, :] - source_xyz[1][:, :, None])
    dist_sq = dist_sq + jnp.square(gas_xyz[2][:, None, :] - source_xyz[2][:, :, None])
    weight = masses[:, None, :] / jnp.square(1.0 + dist_sq * inv_square[:, :, None])
    norm_sum = jnp.sum(weight, axis=2)
    coeffs = load * (live / norm_sum)[None, :, :]
    moved = jnp.einsum("qgs,gsn->qgn", coeffs, weight, precision=lax.Precision.HIGHEST)
    return moved.reshape(load.shape[0], width * tile_ids.shape[1], 128)


def local(
    gas_pos,
    gas_mass,
    source_pos,
    source_radius,
    source_yield,
    source_momentum,
    source_tiles,
    source_count,
):
    gas_size = gas_pos.shape[-1]
    tiles_here = gas_size // 128
    blocks = source_pos.shape[-1] // 128
    listed = source_tiles.shape[-1]
    gas_both = jnp.concatenate([gas_pos, gas_mass[None]], axis=0)
    padded = padded_2(gas_both, (("gz", 3), ("gy", 2), ("gx", 1)), 1)
    near = padded.reshape(4, 27 * tiles_here, 128)
    source_xyz = source_pos.reshape(3, blocks, 128)
    inv_sq = (1.0 / jnp.square(source_radius)).reshape(blocks, 128)
    loads = jnp.concatenate(
        [source_yield[0:1], source_momentum, source_yield[1:2]], axis=0
    ).reshape(5, blocks, 128)
    tile_table = source_tiles.reshape(blocks, listed)
    live_count = source_count.reshape(())
    group = math.gcd(blocks, 4)
    used_blocks = (live_count + 127) // 128
    turns = (used_blocks + group - 1) // group

    def add_group(turn, acc):
        first = turn * group
        live = (
            (first * 128 + lax.iota(jnp.int32, group * 128) < live_count)
            .astype(jnp.float32)
            .reshape(group, 128)
        )
        ids = lax.dynamic_slice_in_dim(tile_table, first, group, 0)
        xyz_rows = lax.dynamic_slice_in_dim(source_xyz, first, group, 1)
        inv_rows = lax.dynamic_slice_in_dim(inv_sq, first, group, 0)
        load_rows = lax.dynamic_slice_in_dim(loads, first, group, 1)
        moved = group_deposit(near, ids, xyz_rows, inv_rows, load_rows, live, tiles_here)
        return acc.at[:, ids.reshape(-1)].add(moved)

    acc_init = jnp.zeros((5, 27 * tiles_here, 128), jnp.float32)
    acc = lax.fori_loop(0, turns, add_group, acc_init)
    spread = acc.reshape(5, 3, 3, 3, gas_size)
    summed = spread
    for axis in ("gx", "gy", "gz"):
        summed = folded(summed, axis)
    gained = summed / gas_mass.reshape(1, gas_size)
    return gained.reshape(5, 1, 1, 1, gas_size)


def solution(mesh):
    in_specs = (
        P(None, "gx", "gy", "gz", None),
        P("gx", "gy", "gz", None),
        P(None, "gx", "gy", "gz", None),
        P("gx", "gy", "gz", None),
        P(None, "gx", "gy", "gz", None),
        P(None, "gx", "gy", "gz", None),
        P("gx", "gy", "gz", None, None),
        P("gx", "gy", "gz"),
    )
    out_specs = P(None, "gx", "gy", "gz", None)
    return jax.shard_map(local, mesh=mesh, in_specs=in_specs, out_specs=out_specs, check_vma=False)
```

```python
import jax
import jax.numpy as jnp
from jax import lax
from jax.experimental import pallas as pl
from jax.experimental.pallas import tpu as pltpu
from jax.sharding import PartitionSpec as P

TILES = 16
BLOCKS = 16
LISTED = 8
GAS_ROWS = 4 * TILES
TABLE_ROW = GAS_ROWS + 9 * BLOCKS
ROWS = TABLE_ROW + LISTED
DEP_ROWS = 5 * TILES
CAP = 8 * BLOCKS + 2
TOGETHER = 2


def shifted(value, axis, step):
    count = lax.axis_size(axis)
    return lax.ppermute(value, axis, [(i, (i + step) % count) for i in range(count)])


def deposit_kernel(near_ref, far_ref, out_near, out_far, tab_v, tab_s, stage, entries, gas, acc, cols, split, sem):
    packets = [(near_ref if o < 4 else far_ref, (o % 4) * ROWS) for o in range(8)]

    for o, (ref, base) in enumerate(packets):
        ids = ref[pl.ds(base + TABLE_ROW, LISTED), :].astype(jnp.int32)
        word = ids[0:1] & 15
        for j in range(1, LISTED):
            word = word | ((ids[j : j + 1] & 15) << (4 * j))
        lane = lax.broadcasted_iota(jnp.int32, (1, 128), 1)
        tab_v[o : o + 1, :] = word
        tab_v[8 + o : 9 + o, :] = jnp.where(lane < BLOCKS, ids[0:1] >> 4, ids[0:1])
    copy = pltpu.make_async_copy(tab_v, tab_s, sem)
    copy.start()
    acc[...] = jnp.zeros_like(acc)
    for j, (ref, base) in enumerate(packets):
        for axis, bit in enumerate((j // 4, j // 2 % 2, j % 2)):
            rows = ref[pl.ds(base + axis * TILES, TILES), :]
            gas[axis, j * TILES : (j + 1) * TILES, :] = rows + float(bit) if bit else rows
        gas[3, j * TILES : (j + 1) * TILES, :] = ref[pl.ds(base + 3 * TILES, TILES), :]
    copy.wait()

    n = jnp.int32(0)
    for o, (ref, base) in enumerate(packets):
        bits = (o // 4, o // 2 % 2, o % 2)
        wanted = 9 * (1 - bits[0]) + 3 * (1 - bits[1]) + (1 - bits[2])
        count = tab_s[8 + o, BLOCKS]

        def look(b, n, o=o, ref=ref, base=base, bits=bits, wanted=wanted, count=count):
            mine = tab_s[8 + o, b] == wanted

            @pl.when(mine)
            def _():
                first = base + GAS_ROWS + b
                for axis in range(3):
                    row = ref[pl.ds(first + axis * BLOCKS, 1), :]
                    stage[n, axis : axis + 1, :] = row + float(bits[axis]) if bits[axis] else row
                radius = ref[pl.ds(first + 3 * BLOCKS, 1), :]
                stage[n, 3:4, :] = radius * radius
                stage[n, 8:16, :] = jnp.zeros((8, 128), jnp.float32)
                for q in range(5):
                    row = first + (4 + (0, 2, 3, 4, 1)[q]) * BLOCKS
                    stage[n, 8 + q : 9 + q, :] = ref[pl.ds(row, 1), :]
                entries[2 * n] = tab_s[o, b]
                entries[2 * n + 1] = count - 128 * b

            return n + mine.astype(jnp.int32)

        n = lax.fori_loop(0, (count + 127) // 128, look, n)

    @pl.when(n % 2 == 1)
    def _():
        stage[n] = stage[n - 1]
        entries[2 * n] = entries[2 * n - 2]
        entries[2 * n + 1] = 0

    def weights(u, e):
        word = entries[2 * e]
        tiles = [(word >> (4 * j)) & 15 for j in range(LISTED)]
        cols[u] = stage[e].T
        at = [[gas[f, pl.ds(j * TILES + tiles[j], 1), :] for f in range(4)] for j in range(LISTED)]
        norms = []
        for p in range(8):
            x, y, z, r2 = (
                jnp.broadcast_to(cols[u, 16 * p : 16 * p + 16, f : f + 1], (16, 128)) for f in range(4)
            )
            total = None
            for j in range(LISTED):
                dx, dy, dz = at[j][0] - x, at[j][1] - y, at[j][2] - z
                q = dx * dx + dy * dy + (dz * dz + r2)
                k = 1.0 / (q * q)
                mk = at[j][3] * k
                total = mk if total is None else total + mk
                high = k.astype(jnp.bfloat16)
                split[u, 16 * p : 16 * p + 16, 128 * j : 128 * j + 128] = high
                low = (k - high.astype(jnp.float32)).astype(jnp.bfloat16)
                split[u, 128 + 16 * p : 144 + 16 * p, 128 * j : 128 * j + 128] = low
            norms.append(total)
        norm = jnp.sum(jnp.concatenate(norms, axis=0).T, axis=0, keepdims=True)
        return tiles, norm

    def deposits(u, e, norm):
        lane = lax.broadcasted_iota(jnp.int32, (8, 128), 1)
        coeff = jnp.where(lane < entries[2 * e + 1], stage[e, 8:16, :] / norm, 0.0)
        high = coeff.astype(jnp.bfloat16)
        low = (coeff - high.astype(jnp.float32)).astype(jnp.bfloat16)
        left = jnp.concatenate(
            [jnp.concatenate([high, high], axis=1), jnp.concatenate([low, jnp.zeros_like(low)], axis=1)], axis=0
        )
        both = jnp.dot(left, split[u], preferred_element_type=jnp.float32)
        return both[0:8] + both[8:16]

    def turn(i, carry):
        done = [weights(u, TOGETHER * i + u) for u in range(TOGETHER)]
        moved = [deposits(u, TOGETHER * i + u, done[u][1]) for u in range(TOGETHER)]
        for u in range(TOGETHER):
            for j in range(LISTED):
                t = j * TILES + done[u][0][j]
                acc[t] = acc[t] + moved[u][:, 128 * j : 128 * j + 128]
        return carry

    lax.fori_loop(0, (n + TOGETHER - 1) // TOGETHER, turn, 0)
    for o in range(8):
        out = out_near if o < 4 else out_far
        for q in range(5):
            row = (o % 4) * DEP_ROWS + q * TILES
            out[row : row + TILES, :] = acc[o * TILES : (o + 1) * TILES, q, :]


def deposits_of(near, far):
    vmem = pl.BlockSpec(memory_space=pltpu.VMEM)
    out = jax.ShapeDtypeStruct((4 * DEP_ROWS, 128), jnp.float32)
    return pl.pallas_call(
        deposit_kernel,
        out_shape=(out, out),
        in_specs=[vmem, vmem],
        out_specs=(vmem, vmem),
        scratch_shapes=[
            pltpu.VMEM((16, 128), jnp.int32),
            pltpu.SMEM((16, 128), jnp.int32),
            pltpu.VMEM((CAP, 16, 128), jnp.float32),
            pltpu.SMEM((2 * CAP,), jnp.int32),
            pltpu.VMEM((4, 8 * TILES, 128), jnp.float32),
            pltpu.VMEM((8 * TILES, 8, 128), jnp.float32),
            pltpu.VMEM((TOGETHER, 128, 16), jnp.float32),
            pltpu.VMEM((TOGETHER, 256, 1024), jnp.bfloat16),
            pltpu.SemaphoreType.DMA,
        ],
    )(near, far)


def local(gas_pos, gas_mass, source_pos, source_radius, source_yield, source_momentum, source_tiles, source_count):
    table = source_tiles.reshape(BLOCKS, LISTED).T.astype(jnp.float32)
    counts = jnp.broadcast_to(source_count.astype(jnp.float32).reshape(1, 1), (LISTED, 128 - BLOCKS))
    packet = jnp.concatenate(
        [
            gas_pos.reshape(3 * TILES, 128),
            gas_mass.reshape(TILES, 128),
            source_pos.reshape(3 * BLOCKS, 128),
            source_radius.reshape(BLOCKS, 128),
            source_yield.reshape(2 * BLOCKS, 128),
            source_momentum.reshape(3 * BLOCKS, 128),
            jnp.concatenate([table, counts], axis=1),
        ],
        axis=0,
    )
    packet = jnp.concatenate([packet, shifted(packet, "gz", -1)], axis=0)
    packet = jnp.concatenate([packet, shifted(packet, "gy", -1)], axis=0)
    near, far = deposits_of(packet, shifted(packet, "gx", -1))
    total = near + shifted(far, "gx", 1)
    half = 2 * DEP_ROWS
    total = total[:half] + shifted(total[half:], "gy", 1)
    total = total[:DEP_ROWS] + shifted(total[DEP_ROWS:], "gz", 1)
    return total.reshape(5, 1, 1, 1, TILES * 128)


def solution(mesh):
    in_specs = (
        P(None, "gx", "gy", "gz", None),
        P("gx", "gy", "gz", None),
        P(None, "gx", "gy", "gz", None),
        P("gx", "gy", "gz", None),
        P(None, "gx", "gy", "gz", None),
        P(None, "gx", "gy", "gz", None),
        P("gx", "gy", "gz", None, None),
        P("gx", "gy", "gz"),
    )
    out_specs = P(None, "gx", "gy", "gz", None)
    return jax.shard_map(local, mesh=mesh, in_specs=in_specs, out_specs=out_specs, check_vma=False)
```

```python
import math

import jax
import jax.numpy as jnp
from jax import lax
from jax.experimental import pallas as pl
from jax.experimental.pallas import tpu as pltpu
from jax.sharding import PartitionSpec as P

TILES = 16
BLOCKS = 16
LISTED = 8
GAS_ROWS = 4 * TILES
TABLE_ROW = GAS_ROWS + 9 * BLOCKS
ROWS = TABLE_ROW + LISTED
DEP_ROWS = 5 * TILES
CAP = 8 * BLOCKS + 2
TOGETHER = 2


def shifted(value, axes, step):
    sizes = [lax.axis_size(axis) for axis in axes]
    pairs = []
    for source in range(math.prod(sizes)):
        rest, target, scale = source, 0, 1
        for size in reversed(sizes):
            target += (rest % size + step) % size * scale
            rest, scale = rest // size, scale * size
        pairs.append((source, target))
    return lax.ppermute(value, axes, pairs)


def pack_kernel(pos, mass, s_pos, s_radius, s_yield, s_momentum, tiles, count, out, table, sems):
    copies = [pltpu.make_async_copy(tiles, table, sems.at[6])]
    row = 0
    for i, part in enumerate((pos, mass, s_pos, s_radius, s_yield, s_momentum)):
        copies.append(pltpu.make_async_copy(part, out.at[pl.ds(row, part.shape[0])], sems.at[i]))
        row += part.shape[0]
    for copy in copies:
        copy.start()
    copies[0].wait()
    out[row:, :] = jnp.full((LISTED, 128), count[0, 0].astype(jnp.float32))
    out[row:, :BLOCKS] = table[...].astype(jnp.float32)
    for copy in copies[1:]:
        copy.wait()


def packed(parts, tiles, count):
    hbm = pl.BlockSpec(memory_space=pltpu.HBM)
    return pl.pallas_call(
        pack_kernel,
        out_shape=jax.ShapeDtypeStruct((ROWS, 128), jnp.float32),
        in_specs=[hbm] * 7 + [pl.BlockSpec(memory_space=pltpu.SMEM)],
        out_specs=pl.BlockSpec(memory_space=pltpu.VMEM),
        compiler_params=pltpu.CompilerParams(vmem_limit_bytes=2 << 20),
        scratch_shapes=[
            pltpu.VMEM((LISTED, BLOCKS), jnp.int32),
            pltpu.SemaphoreType.DMA((7,)),
        ],
    )(*(pltpu.with_memory_space_constraint(part, pltpu.HBM) for part in (*parts, tiles)), count)


def deposit_kernel(in_0, in_y, in_x, in_xy, out_0, out_y, out_x, out_xy, tab_v, tab_s, stage, entries, gas, acc, cols, split, sem):
    packets = [((in_0, in_y, in_x, in_xy)[o // 2], o % 2 * ROWS) for o in range(8)]

    for o, (ref, base) in enumerate(packets):
        ids = ref[pl.ds(base + TABLE_ROW, LISTED), :].astype(jnp.int32)
        word = ids[0:1] & 15
        for j in range(1, LISTED):
            word = word | ((ids[j : j + 1] & 15) << (4 * j))
        lane = lax.broadcasted_iota(jnp.int32, (1, 128), 1)
        tab_v[o : o + 1, :] = word
        tab_v[8 + o : 9 + o, :] = jnp.where(lane < BLOCKS, ids[0:1] >> 4, ids[0:1])
    copy = pltpu.make_async_copy(tab_v, tab_s, sem)
    copy.start()
    acc[...] = jnp.zeros_like(acc)
    for j, (ref, base) in enumerate(packets):
        for axis, bit in enumerate((j // 4, j // 2 % 2, j % 2)):
            rows = ref[pl.ds(base + axis * TILES, TILES), :]
            gas[axis, j * TILES : (j + 1) * TILES, :] = rows + float(bit) if bit else rows
        gas[3, j * TILES : (j + 1) * TILES, :] = ref[pl.ds(base + 3 * TILES, TILES), :]
    copy.wait()

    n = jnp.int32(0)
    for o, (ref, base) in enumerate(packets):
        bits = (o // 4, o // 2 % 2, o % 2)
        wanted = 9 * (1 - bits[0]) + 3 * (1 - bits[1]) + (1 - bits[2])
        count = tab_s[8 + o, BLOCKS]

        def look(b, n, o=o, ref=ref, base=base, bits=bits, wanted=wanted, count=count):
            mine = tab_s[8 + o, b] == wanted

            @pl.when(mine)
            def _():
                first = base + GAS_ROWS + b
                for axis in range(3):
                    row = ref[pl.ds(first + axis * BLOCKS, 1), :]
                    stage[n, axis : axis + 1, :] = row + float(bits[axis]) if bits[axis] else row
                radius = ref[pl.ds(first + 3 * BLOCKS, 1), :]
                stage[n, 3:4, :] = radius * radius
                stage[n, 8:16, :] = jnp.zeros((8, 128), jnp.float32)
                for q in range(5):
                    row = first + (4 + (0, 2, 3, 4, 1)[q]) * BLOCKS
                    stage[n, 8 + q : 9 + q, :] = ref[pl.ds(row, 1), :]
                entries[2 * n] = tab_s[o, b]
                entries[2 * n + 1] = count - 128 * b

            return n + mine.astype(jnp.int32)

        n = lax.fori_loop(0, (count + 127) // 128, look, n)

    @pl.when(n % 2 == 1)
    def _():
        stage[n] = stage[n - 1]
        entries[2 * n] = entries[2 * n - 2]
        entries[2 * n + 1] = 0

    def weights(u, e):
        word = entries[2 * e]
        tiles = [(word >> (4 * j)) & 15 for j in range(LISTED)]
        cols[u] = stage[e].T
        at = [[gas[f, pl.ds(j * TILES + tiles[j], 1), :] for f in range(4)] for j in range(LISTED)]
        norms = []
        for p in range(8):
            x, y, z, r2 = (
                jnp.broadcast_to(cols[u, 16 * p : 16 * p + 16, f : f + 1], (16, 128)) for f in range(4)
            )
            total = None
            for j in range(LISTED):
                dx, dy, dz = at[j][0] - x, at[j][1] - y, at[j][2] - z
                q = dx * dx + dy * dy + (dz * dz + r2)
                k = 1.0 / (q * q)
                mk = at[j][3] * k
                total = mk if total is None else total + mk
                high = k.astype(jnp.bfloat16)
                split[u, 16 * p : 16 * p + 16, 128 * j : 128 * j + 128] = high
                low = (k - high.astype(jnp.float32)).astype(jnp.bfloat16)
                split[u, 128 + 16 * p : 144 + 16 * p, 128 * j : 128 * j + 128] = low
            norms.append(total)
        norm = jnp.sum(jnp.concatenate(norms, axis=0).T, axis=0, keepdims=True)
        return tiles, norm

    def deposits(u, e, norm):
        lane = lax.broadcasted_iota(jnp.int32, (8, 128), 1)
        coeff = jnp.where(lane < entries[2 * e + 1], stage[e, 8:16, :] / norm, 0.0)
        high = coeff.astype(jnp.bfloat16)
        low = (coeff - high.astype(jnp.float32)).astype(jnp.bfloat16)
        left = jnp.concatenate(
            [jnp.concatenate([high, high], axis=1), jnp.concatenate([low, jnp.zeros_like(low)], axis=1)], axis=0
        )
        both = jnp.dot(left, split[u], preferred_element_type=jnp.float32)
        return both[0:8] + both[8:16]

    def turn(i, carry):
        done = [weights(u, TOGETHER * i + u) for u in range(TOGETHER)]
        moved = [deposits(u, TOGETHER * i + u, done[u][1]) for u in range(TOGETHER)]
        for u in range(TOGETHER):
            for j in range(LISTED):
                t = j * TILES + done[u][0][j]
                acc[t] = acc[t] + moved[u][:, 128 * j : 128 * j + 128]
        return carry

    lax.fori_loop(0, (n + TOGETHER - 1) // TOGETHER, turn, 0)
    for o in range(8):
        out = (out_0, out_y, out_x, out_xy)[o // 2]
        for q in range(5):
            row = o % 2 * DEP_ROWS + q * TILES
            out[row : row + TILES, :] = acc[o * TILES : (o + 1) * TILES, q, :]


def deposits_of(packets):
    vmem = pl.BlockSpec(memory_space=pltpu.VMEM)
    out = jax.ShapeDtypeStruct((2 * DEP_ROWS, 128), jnp.float32)
    return pl.pallas_call(
        deposit_kernel,
        out_shape=(out,) * 4,
        in_specs=[vmem] * 4,
        out_specs=(vmem,) * 4,
        compiler_params=pltpu.CompilerParams(vmem_limit_bytes=16 << 20),
        scratch_shapes=[
            pltpu.VMEM((16, 128), jnp.int32),
            pltpu.SMEM((16, 128), jnp.int32),
            pltpu.VMEM((CAP, 16, 128), jnp.float32),
            pltpu.SMEM((2 * CAP,), jnp.int32),
            pltpu.VMEM((4, 8 * TILES, 128), jnp.float32),
            pltpu.VMEM((8 * TILES, 8, 128), jnp.float32),
            pltpu.VMEM((TOGETHER, 128, 16), jnp.float32),
            pltpu.VMEM((TOGETHER, 256, 1024), jnp.bfloat16),
            pltpu.SemaphoreType.DMA,
        ],
    )(*packets)


def local(gas_pos, gas_mass, source_pos, source_radius, source_yield, source_momentum, source_tiles, source_count):
    parts = (gas_pos, gas_mass, source_pos, source_radius, source_yield, source_momentum)
    parts = [part.reshape(-1, 128) for part in parts]
    packet = packed(parts, source_tiles.reshape(BLOCKS, LISTED).T, source_count.reshape(1, 1))
    packet = jnp.concatenate([packet, shifted(packet, ("gz",), -1)], axis=0)
    sides = (("gx", "gy"), ("gy",), ("gx",))
    far = [shifted(packet, axes, -1) for axes in sides]
    own, *outward = deposits_of((packet, far[1], far[2], far[0]))
    outward = (outward[2], outward[0], outward[1])
    back = [shifted(part, axes, 1) for part, axes in zip(outward, sides)]
    total = own + back[0] + back[1] + back[2]
    total = total[:DEP_ROWS] + shifted(total[DEP_ROWS:], ("gz",), 1)
    return total.reshape(5, 1, 1, 1, TILES * 128)


def solution(mesh):
    in_specs = (
        P(None, "gx", "gy", "gz", None),
        P("gx", "gy", "gz", None),
        P(None, "gx", "gy", "gz", None),
        P("gx", "gy", "gz", None),
        P(None, "gx", "gy", "gz", None),
        P(None, "gx", "gy", "gz", None),
        P("gx", "gy", "gz", None, None),
        P("gx", "gy", "gz"),
    )
    out_specs = P(None, "gx", "gy", "gz", None)
    return jax.shard_map(local, mesh=mesh, in_specs=in_specs, out_specs=out_specs, check_vma=False)
```

```python
import math

import jax
import jax.numpy as jnp
from jax import lax
from jax.experimental import pallas as pl
from jax.experimental.pallas import tpu as pltpu
from jax.sharding import PartitionSpec as P

TILES = 16
BLOCKS = 16
LISTED = 8
GAS_ROWS = 4 * TILES
TABLE_ROW = GAS_ROWS + 9 * BLOCKS
ROWS = TABLE_ROW + LISTED
DEP_ROWS = 5 * TILES
CAP = 8 * BLOCKS + 4
TOGETHER = 2


def shifted(value, axes, step):
    sizes = [lax.axis_size(axis) for axis in axes]
    pairs = []
    for source in range(math.prod(sizes)):
        rest, target, scale = source, 0, 1
        for size in reversed(sizes):
            target += (rest % size + step) % size * scale
            rest, scale = rest // size, scale * size
        pairs.append((source, target))
    return lax.ppermute(value, axes, pairs)


def pack_kernel(pos, mass, s_pos, s_radius, s_yield, s_momentum, tiles, count, out, table, sems):
    copies = [pltpu.make_async_copy(tiles, table, sems.at[6])]
    row = 0
    for i, part in enumerate((pos, mass, s_pos, s_radius, s_yield, s_momentum)):
        copies.append(pltpu.make_async_copy(part, out.at[pl.ds(row, part.shape[0])], sems.at[i]))
        row += part.shape[0]
    for copy in copies:
        copy.start()
    copies[0].wait()
    out[row:, :] = jnp.full((LISTED, 128), count[0, 0].astype(jnp.float32))
    out[row:, :BLOCKS] = table[...].astype(jnp.float32)
    for copy in copies[1:]:
        copy.wait()


def packed(parts, tiles, count):
    hbm = pl.BlockSpec(memory_space=pltpu.HBM)
    return pl.pallas_call(
        pack_kernel,
        out_shape=jax.ShapeDtypeStruct((ROWS, 128), jnp.float32),
        in_specs=[hbm] * 7 + [pl.BlockSpec(memory_space=pltpu.SMEM)],
        out_specs=pl.BlockSpec(memory_space=pltpu.VMEM),
        compiler_params=pltpu.CompilerParams(vmem_limit_bytes=2 << 20),
        scratch_shapes=[
            pltpu.VMEM((LISTED, BLOCKS), jnp.int32),
            pltpu.SemaphoreType.DMA((7,)),
        ],
    )(*(pltpu.with_memory_space_constraint(part, pltpu.HBM) for part in (*parts, tiles)), count)


def three(v):
    first = v.astype(jnp.bfloat16).astype(jnp.float32)
    rest = v - first
    second = rest.astype(jnp.bfloat16).astype(jnp.float32)
    return first, second, rest - second


def deposit_kernel(
    in_0, in_y, in_x, in_xy, out_0, out_y, out_x, out_xy, tab_v, tab_s, stage, loads, entries, acc, split, sem
):
    packets = [((in_0, in_y, in_x, in_xy)[o // 2], o % 2 * ROWS) for o in range(8)]
    row = lax.broadcasted_iota(jnp.int32, (8, 128), 0)
    lane = lax.broadcasted_iota(jnp.int32, (8, 128), 1)

    def centred(o):
        shift = jnp.zeros((8, 128), jnp.float32)
        for axis, bit in enumerate((o // 4, o // 2 % 2, o % 2)):
            if not bit:
                shift = jnp.where(row == axis, -1.0, shift)
        return shift

    for o, (ref, base) in enumerate(packets):
        ids = ref[pl.ds(base + TABLE_ROW, LISTED), :].astype(jnp.int32)
        word = ids[0:1] & 15
        for j in range(1, LISTED):
            word = word | ((ids[j : j + 1] & 15) << (4 * j))
        tab_v[o : o + 1, :] = word
        tab_v[8 + o : 9 + o, :] = jnp.where(lane[0:1] < BLOCKS, ids[0:1] >> 4, ids[0:1])
    copy = pltpu.make_async_copy(tab_v, tab_s, sem)
    copy.start()
    acc[...] = jnp.zeros_like(acc)
    copy.wait()

    n = jnp.int32(0)
    for o, (ref, base) in enumerate(packets):
        wanted = 9 * (1 - o // 4) + 3 * (1 - o // 2 % 2) + (1 - o % 2)
        count = tab_s[8 + o, BLOCKS]
        shift = centred(o)

        def look(b, n, o=o, ref=ref, base=base, wanted=wanted, count=count, shift=shift):
            first = base + GAS_ROWS + b
            stage[n] = ref[pl.ds(first, 8, stride=BLOCKS), :] + shift
            loads[n, 0:5, :] = ref[pl.ds(first + 4 * BLOCKS, 5, stride=BLOCKS), :]
            entries[2 * n] = tab_s[o, b]
            entries[2 * n + 1] = count - 128 * b
            return n + (tab_s[8 + o, b] == wanted).astype(jnp.int32)

        n = lax.fori_loop(0, (count + 127) // 128, look, n)

    for extra in range(TOGETHER - 1):
        stage[n + extra] = stage[0]
        loads[n + extra] = loads[0]
        entries[2 * (n + extra)] = entries[0]
        entries[2 * (n + extra) + 1] = 0

    def weights(u, e):
        word = entries[2 * e]
        tiles = [(word >> (4 * j)) & 15 for j in range(LISTED)]
        s = stage[e]
        square = jnp.sum(jnp.where(row < 4, s * s, 0.0), axis=0, keepdims=True)
        s = jnp.where(row < 3, s, jnp.where(row == 3, square, jnp.where(row == 4, 1.0, 0.0)))
        a, b, c = three(s)
        left = jnp.concatenate([a, a, b, b, a, c], axis=0).T
        norms = [None] * 8
        for pair in range(LISTED // 2):
            rights, masses = [], []
            for j in (2 * pair, 2 * pair + 1):
                ref, base = packets[j]
                g = ref[pl.ds(base + tiles[j], 8, stride=TILES), :]
                masses.append(g[3:4])
                g = g + centred(j)
                square = jnp.sum(jnp.where(row < 3, g * g, 0.0), axis=0, keepdims=True)
                g = jnp.where(row < 3, -2.0 * g, jnp.where(row == 3, 1.0, jnp.where(row == 4, square, 0.0)))
                a, b, c = three(g)
                rights.append(jnp.concatenate([a, b, a, b, c, a], axis=0))
            q = jnp.dot(left, jnp.concatenate(rights, axis=1), preferred_element_type=jnp.float32)
            for p in range(8):
                for h in range(2):
                    part = q[16 * p : 16 * p + 16, 128 * h : 128 * h + 128]
                    k = 1.0 / (part * part)
                    mk = masses[h] * k
                    norms[p] = mk if norms[p] is None else norms[p] + mk
                    scaled = k * 65537.0
                    high = scaled - (scaled - k)
                    at = 256 * pair + 128 * h
                    split[u, 16 * p : 16 * p + 16, at : at + 128] = high
                    split[u, 128 + 16 * p : 144 + 16 * p, at : at + 128] = k - high
        norm = jnp.sum(jnp.concatenate(norms, axis=0).T, axis=0, keepdims=True)
        return tiles, norm

    def deposits(u, e, norm):
        coeff = jnp.where((lane < entries[2 * e + 1]) & (row < 5), loads[e] / norm, 0.0)
        high = coeff.astype(jnp.bfloat16).astype(jnp.float32)
        low = coeff - high
        left = jnp.concatenate(
            [jnp.concatenate([high, high], axis=1), jnp.concatenate([low, jnp.zeros_like(low)], axis=1)], axis=0
        )
        both = jnp.dot(left, split[u], preferred_element_type=jnp.float32)
        return both[0:8] + both[8:16]

    def turn(i, carry):
        done = [weights(u, TOGETHER * i + u) for u in range(TOGETHER)]
        moved = [deposits(u, TOGETHER * i + u, done[u][1]) for u in range(TOGETHER)]
        for u in range(TOGETHER):
            for j in range(LISTED):
                t = j * TILES + done[u][0][j]
                acc[t] = acc[t] + moved[u][:, 128 * j : 128 * j + 128]
        return carry

    lax.fori_loop(0, (n + TOGETHER - 1) // TOGETHER, turn, 0)
    for o in range(8):
        out = (out_0, out_y, out_x, out_xy)[o // 2]
        for q, source in enumerate((0, 2, 3, 4, 1)):
            at = o % 2 * DEP_ROWS + q * TILES
            out[at : at + TILES, :] = acc[o * TILES : (o + 1) * TILES, source, :]


def deposits_of(packets):
    vmem = pl.BlockSpec(memory_space=pltpu.VMEM)
    out = jax.ShapeDtypeStruct((2 * DEP_ROWS, 128), jnp.float32)
    return pl.pallas_call(
        deposit_kernel,
        out_shape=(out,) * 4,
        in_specs=[vmem] * 4,
        out_specs=(vmem,) * 4,
        compiler_params=pltpu.CompilerParams(vmem_limit_bytes=16 << 20),
        scratch_shapes=[
            pltpu.VMEM((16, 128), jnp.int32),
            pltpu.SMEM((16, 128), jnp.int32),
            pltpu.VMEM((CAP, 8, 128), jnp.float32),
            pltpu.VMEM((CAP, 8, 128), jnp.float32),
            pltpu.SMEM((2 * CAP,), jnp.int32),
            pltpu.VMEM((8 * TILES, 8, 128), jnp.float32),
            pltpu.VMEM((TOGETHER, 256, 1024), jnp.float32),
            pltpu.SemaphoreType.DMA,
        ],
    )(*packets)


def local(gas_pos, gas_mass, source_pos, source_radius, source_yield, source_momentum, source_tiles, source_count):
    parts = (gas_pos, gas_mass, source_pos, source_radius, source_yield, source_momentum)
    parts = [part.reshape(-1, 128) for part in parts]
    packet = packed(parts, source_tiles.reshape(BLOCKS, LISTED).T, source_count.reshape(1, 1))
    packet = jnp.concatenate([packet, shifted(packet, ("gz",), -1)], axis=0)
    sides = (("gx", "gy"), ("gy",), ("gx",))
    far = [shifted(packet, axes, -1) for axes in sides]
    own, *outward = deposits_of((packet, far[1], far[2], far[0]))
    outward = (outward[2], outward[0], outward[1])
    back = [shifted(part, axes, 1) for part, axes in zip(outward, sides)]
    total = own + back[0] + back[1] + back[2]
    total = total[:DEP_ROWS] + shifted(total[DEP_ROWS:], ("gz",), 1)
    return total.reshape(5, 1, 1, 1, TILES * 128)


def solution(mesh):
    in_specs = (
        P(None, "gx", "gy", "gz", None),
        P("gx", "gy", "gz", None),
        P(None, "gx", "gy", "gz", None),
        P("gx", "gy", "gz", None),
        P(None, "gx", "gy", "gz", None),
        P(None, "gx", "gy", "gz", None),
        P("gx", "gy", "gz", None, None),
        P("gx", "gy", "gz"),
    )
    out_specs = P(None, "gx", "gy", "gz", None)
    return jax.shard_map(local, mesh=mesh, in_specs=in_specs, out_specs=out_specs, check_vma=False)
```

```python
import math

import jax
import jax.numpy as jnp
from jax import lax
from jax.experimental import pallas as pl
from jax.experimental.pallas import tpu as pltpu
from jax.sharding import PartitionSpec as P

TILES = 16
BLOCKS = 16
LISTED = 8
GAS_ROWS = 4 * TILES
TABLE_ROW = GAS_ROWS + 9 * BLOCKS
ROWS = TABLE_ROW + LISTED
DEP_ROWS = 5 * TILES
CAP = 8 * BLOCKS + 4
TOGETHER = 3


def shifted(value, axes, step):
    sizes = [lax.axis_size(axis) for axis in axes]
    pairs = []
    for source in range(math.prod(sizes)):
        rest, target, scale = source, 0, 1
        for size in reversed(sizes):
            target += (rest % size + step) % size * scale
            rest, scale = rest // size, scale * size
        pairs.append((source, target))
    return lax.ppermute(value, axes, pairs)


def pack_kernel(pos, mass, s_pos, s_radius, s_yield, s_momentum, tiles, count, out, table, sems):
    copies = [pltpu.make_async_copy(tiles, table, sems.at[6])]
    row = 0
    for i, part in enumerate((pos, mass, s_pos, s_radius, s_yield, s_momentum)):
        copies.append(pltpu.make_async_copy(part, out.at[pl.ds(row, part.shape[0])], sems.at[i]))
        row += part.shape[0]
    for copy in copies:
        copy.start()
    copies[0].wait()
    out[row:, :] = jnp.full((LISTED, 128), count[0, 0].astype(jnp.float32))
    out[row:, :BLOCKS] = table[...].astype(jnp.float32)
    for copy in copies[1:]:
        copy.wait()


def packed(parts, tiles, count):
    hbm = pl.BlockSpec(memory_space=pltpu.HBM)
    return pl.pallas_call(
        pack_kernel,
        out_shape=jax.ShapeDtypeStruct((ROWS, 128), jnp.float32),
        in_specs=[hbm] * 7 + [pl.BlockSpec(memory_space=pltpu.SMEM)],
        out_specs=pl.BlockSpec(memory_space=pltpu.VMEM),
        compiler_params=pltpu.CompilerParams(vmem_limit_bytes=2 << 20),
        scratch_shapes=[
            pltpu.VMEM((LISTED, BLOCKS), jnp.int32),
            pltpu.SemaphoreType.DMA((7,)),
        ],
    )(*(pltpu.with_memory_space_constraint(part, pltpu.HBM) for part in (*parts, tiles)), count)


def three(v):
    first = v.astype(jnp.bfloat16).astype(jnp.float32)
    rest = v - first
    second = rest.astype(jnp.bfloat16).astype(jnp.float32)
    return first, second, rest - second


def deposit_kernel(
    in_0, in_y, in_x, in_xy, out_0, out_y, out_x, out_xy, tab_v, tab_s, stage, loads, entries, acc, split, sem
):
    packets = [((in_0, in_y, in_x, in_xy)[o // 2], o % 2 * ROWS) for o in range(8)]
    row = lax.broadcasted_iota(jnp.int32, (8, 128), 0)
    lane = lax.broadcasted_iota(jnp.int32, (8, 128), 1)

    def centred(o):
        shift = jnp.zeros((8, 128), jnp.float32)
        for axis, bit in enumerate((o // 4, o // 2 % 2, o % 2)):
            if not bit:
                shift = jnp.where(row == axis, -1.0, shift)
        return shift

    for o, (ref, base) in enumerate(packets):
        ids = ref[pl.ds(base + TABLE_ROW, LISTED), :].astype(jnp.int32)
        word = ids[0:1] & 15
        for j in range(1, LISTED):
            word = word | ((ids[j : j + 1] & 15) << (4 * j))
        tab_v[o : o + 1, :] = word
        tab_v[8 + o : 9 + o, :] = jnp.where(lane[0:1] < BLOCKS, ids[0:1] >> 4, ids[0:1])
    copy = pltpu.make_async_copy(tab_v, tab_s, sem)
    copy.start()
    acc[...] = jnp.zeros_like(acc)
    copy.wait()

    n = jnp.int32(0)
    for o, (ref, base) in enumerate(packets):
        wanted = 9 * (1 - o // 4) + 3 * (1 - o // 2 % 2) + (1 - o % 2)
        count = tab_s[8 + o, BLOCKS]
        shift = centred(o)

        def look(b, n, o=o, ref=ref, base=base, wanted=wanted, count=count, shift=shift):
            first = base + GAS_ROWS + b
            stage[n] = ref[pl.ds(first, 8, stride=BLOCKS), :] + shift
            loads[n, 0:5, :] = ref[pl.ds(first + 4 * BLOCKS, 5, stride=BLOCKS), :]
            entries[2 * n] = tab_s[o, b]
            entries[2 * n + 1] = count - 128 * b
            return n + (tab_s[8 + o, b] == wanted).astype(jnp.int32)

        n = lax.fori_loop(0, (count + 127) // 128, look, n)

    for extra in range(TOGETHER - 1):
        stage[n + extra] = stage[0]
        loads[n + extra] = loads[0]
        entries[2 * (n + extra)] = entries[0]
        entries[2 * (n + extra) + 1] = 0

    def weights(u, e):
        word = entries[2 * e]
        tiles = [(word >> (4 * j)) & 15 for j in range(LISTED)]
        s = stage[e]
        square = jnp.sum(jnp.where(row < 4, s * s, 0.0), axis=0, keepdims=True)
        s = jnp.where(row < 3, s, jnp.where(row == 3, square, jnp.where(row == 4, 1.0, 0.0)))
        a, b, c = three(s)
        left = jnp.concatenate([a, a, b, b, a, c], axis=0).T
        norms = [None] * 8
        for pair in range(LISTED // 2):
            rights, masses = [], []
            for j in (2 * pair, 2 * pair + 1):
                ref, base = packets[j]
                g = ref[pl.ds(base + tiles[j], 8, stride=TILES), :]
                masses.append(g[3:4])
                g = g + centred(j)
                square = jnp.sum(jnp.where(row < 3, g * g, 0.0), axis=0, keepdims=True)
                g = jnp.where(row < 3, -2.0 * g, jnp.where(row == 3, 1.0, jnp.where(row == 4, square, 0.0)))
                a, b, c = three(g)
                rights.append(jnp.concatenate([a, b, a, b, c, a], axis=0))
            q = jnp.dot(left, jnp.concatenate(rights, axis=1), preferred_element_type=jnp.float32)
            for p in range(8):
                for h in range(2):
                    part = q[16 * p : 16 * p + 16, 128 * h : 128 * h + 128]
                    k = 1.0 / (part * part)
                    mk = masses[h] * k
                    norms[p] = mk if norms[p] is None else norms[p] + mk
                    scaled = k * 65537.0
                    high = scaled - (scaled - k)
                    at = 256 * pair + 128 * h
                    split[u, 16 * p : 16 * p + 16, at : at + 128] = high
                    split[u, 128 + 16 * p : 144 + 16 * p, at : at + 128] = k - high
        norm = jnp.sum(jnp.concatenate(norms, axis=0).T, axis=0, keepdims=True)
        return tiles, norm

    def deposits(u, e, norm):
        coeff = jnp.where((lane < entries[2 * e + 1]) & (row < 5), loads[e] / norm, 0.0)
        high = coeff.astype(jnp.bfloat16).astype(jnp.float32)
        low = coeff - high
        left = jnp.concatenate(
            [jnp.concatenate([high, high], axis=1), jnp.concatenate([low, jnp.zeros_like(low)], axis=1)], axis=0
        )
        both = jnp.dot(left, split[u], preferred_element_type=jnp.float32)
        return both[0:8] + both[8:16]

    def turn(i, carry):
        done = [weights(u, TOGETHER * i + u) for u in range(TOGETHER)]
        moved = [deposits(u, TOGETHER * i + u, done[u][1]) for u in range(TOGETHER)]
        for u in range(TOGETHER):
            for j in range(LISTED):
                t = j * TILES + done[u][0][j]
                acc[t] = acc[t] + moved[u][:, 128 * j : 128 * j + 128]
        return carry

    lax.fori_loop(0, (n + TOGETHER - 1) // TOGETHER, turn, 0)
    for o in range(8):
        out = (out_0, out_y, out_x, out_xy)[o // 2]
        for q, source in enumerate((0, 2, 3, 4, 1)):
            at = o % 2 * DEP_ROWS + q * TILES
            out[at : at + TILES, :] = acc[o * TILES : (o + 1) * TILES, source, :]


def deposits_of(packets):
    vmem = pl.BlockSpec(memory_space=pltpu.VMEM)
    out = jax.ShapeDtypeStruct((2 * DEP_ROWS, 128), jnp.float32)
    return pl.pallas_call(
        deposit_kernel,
        out_shape=(out,) * 4,
        in_specs=[vmem] * 4,
        out_specs=(vmem,) * 4,
        compiler_params=pltpu.CompilerParams(vmem_limit_bytes=16 << 20),
        scratch_shapes=[
            pltpu.VMEM((16, 128), jnp.int32),
            pltpu.SMEM((16, 128), jnp.int32),
            pltpu.VMEM((CAP, 8, 128), jnp.float32),
            pltpu.VMEM((CAP, 8, 128), jnp.float32),
            pltpu.SMEM((2 * CAP,), jnp.int32),
            pltpu.VMEM((8 * TILES, 8, 128), jnp.float32),
            pltpu.VMEM((TOGETHER, 256, 1024), jnp.float32),
            pltpu.SemaphoreType.DMA,
        ],
    )(*packets)


def local(gas_pos, gas_mass, source_pos, source_radius, source_yield, source_momentum, source_tiles, source_count):
    parts = (gas_pos, gas_mass, source_pos, source_radius, source_yield, source_momentum)
    parts = [part.reshape(-1, 128) for part in parts]
    packet = packed(parts, source_tiles.reshape(BLOCKS, LISTED).T, source_count.reshape(1, 1))
    packet = jnp.concatenate([packet, shifted(packet, ("gz",), -1)], axis=0)
    sides = (("gx", "gy"), ("gy",), ("gx",))
    far = [shifted(packet, axes, -1) for axes in sides]
    own, *outward = deposits_of((packet, far[1], far[2], far[0]))
    outward = (outward[2], outward[0], outward[1])
    back = [shifted(part, axes, 1) for part, axes in zip(outward, sides)]
    total = own + back[0] + back[1] + back[2]
    total = total[:DEP_ROWS] + shifted(total[DEP_ROWS:], ("gz",), 1)
    return total.reshape(5, 1, 1, 1, TILES * 128)


def solution(mesh):
    in_specs = (
        P(None, "gx", "gy", "gz", None),
        P("gx", "gy", "gz", None),
        P(None, "gx", "gy", "gz", None),
        P("gx", "gy", "gz", None),
        P(None, "gx", "gy", "gz", None),
        P(None, "gx", "gy", "gz", None),
        P("gx", "gy", "gz", None, None),
        P("gx", "gy", "gz"),
    )
    out_specs = P(None, "gx", "gy", "gz", None)
    return jax.shard_map(local, mesh=mesh, in_specs=in_specs, out_specs=out_specs, check_vma=False)
```

```python
import math

import jax
import jax.numpy as jnp
from jax import lax
from jax.experimental import pallas as pl
from jax.experimental.pallas import tpu as pltpu
from jax.sharding import PartitionSpec as P

TILES = 16
BLOCKS = 16
LISTED = 8
GAS_ROWS = 4 * TILES
TABLE_ROW = GAS_ROWS + 9 * BLOCKS
ROWS = TABLE_ROW + LISTED
DEP_ROWS = 5 * TILES
CAP = 8 * BLOCKS + 4
TOGETHER = 4


def shifted(value, axes, step):
    sizes = [lax.axis_size(axis) for axis in axes]
    pairs = []
    for source in range(math.prod(sizes)):
        rest, target, scale = source, 0, 1
        for size in reversed(sizes):
            target += (rest % size + step) % size * scale
            rest, scale = rest // size, scale * size
        pairs.append((source, target))
    return lax.ppermute(value, axes, pairs)


def pack_kernel(pos, mass, s_pos, s_radius, s_yield, s_momentum, tiles, count, out, table, sems):
    copies = [pltpu.make_async_copy(tiles, table, sems.at[6])]
    row = 0
    for i, part in enumerate((pos, mass, s_pos, s_radius, s_yield, s_momentum)):
        copies.append(pltpu.make_async_copy(part, out.at[pl.ds(row, part.shape[0])], sems.at[i]))
        row += part.shape[0]
    for copy in copies:
        copy.start()
    copies[0].wait()
    out[row:, :] = jnp.full((LISTED, 128), count[0, 0].astype(jnp.float32))
    out[row:, :BLOCKS] = table[...].astype(jnp.float32)
    for copy in copies[1:]:
        copy.wait()


def packed(parts, tiles, count):
    hbm = pl.BlockSpec(memory_space=pltpu.HBM)
    return pl.pallas_call(
        pack_kernel,
        out_shape=jax.ShapeDtypeStruct((ROWS, 128), jnp.float32),
        in_specs=[hbm] * 7 + [pl.BlockSpec(memory_space=pltpu.SMEM)],
        out_specs=pl.BlockSpec(memory_space=pltpu.VMEM),
        compiler_params=pltpu.CompilerParams(vmem_limit_bytes=2 << 20),
        scratch_shapes=[
            pltpu.VMEM((LISTED, BLOCKS), jnp.int32),
            pltpu.SemaphoreType.DMA((7,)),
        ],
    )(*(pltpu.with_memory_space_constraint(part, pltpu.HBM) for part in (*parts, tiles)), count)


def three(v):
    first = v.astype(jnp.bfloat16).astype(jnp.float32)
    rest = v - first
    second = rest.astype(jnp.bfloat16).astype(jnp.float32)
    return first, second, rest - second


def deposit_kernel(
    in_0, in_y, in_x, in_xy, out_0, out_y, out_x, out_xy, tab_v, tab_s, stage, loads, entries, acc, split, sem
):
    packets = [((in_0, in_y, in_x, in_xy)[o // 2], o % 2 * ROWS) for o in range(8)]
    row = lax.broadcasted_iota(jnp.int32, (8, 128), 0)
    lane = lax.broadcasted_iota(jnp.int32, (8, 128), 1)

    def centred(o):
        shift = jnp.zeros((8, 128), jnp.float32)
        for axis, bit in enumerate((o // 4, o // 2 % 2, o % 2)):
            if not bit:
                shift = jnp.where(row == axis, -1.0, shift)
        return shift

    for o, (ref, base) in enumerate(packets):
        ids = ref[pl.ds(base + TABLE_ROW, LISTED), :].astype(jnp.int32)
        word = ids[0:1] & 15
        for j in range(1, LISTED):
            word = word | ((ids[j : j + 1] & 15) << (4 * j))
        tab_v[o : o + 1, :] = word
        tab_v[8 + o : 9 + o, :] = jnp.where(lane[0:1] < BLOCKS, ids[0:1] >> 4, ids[0:1])
    copy = pltpu.make_async_copy(tab_v, tab_s, sem)
    copy.start()
    acc[...] = jnp.zeros_like(acc)
    copy.wait()

    n = jnp.int32(0)
    for o, (ref, base) in enumerate(packets):
        wanted = 9 * (1 - o // 4) + 3 * (1 - o // 2 % 2) + (1 - o % 2)
        count = tab_s[8 + o, BLOCKS]
        shift = centred(o)

        def look(b, n, o=o, ref=ref, base=base, wanted=wanted, count=count, shift=shift):
            first = base + GAS_ROWS + b
            stage[n] = ref[pl.ds(first, 8, stride=BLOCKS), :] + shift
            loads[n, 0:5, :] = ref[pl.ds(first + 4 * BLOCKS, 5, stride=BLOCKS), :]
            entries[2 * n] = tab_s[o, b]
            entries[2 * n + 1] = count - 128 * b
            return n + (tab_s[8 + o, b] == wanted).astype(jnp.int32)

        n = lax.fori_loop(0, (count + 127) // 128, look, n)

    for extra in range(TOGETHER - 1):
        stage[n + extra] = stage[0]
        loads[n + extra] = loads[0]
        entries[2 * (n + extra)] = entries[0]
        entries[2 * (n + extra) + 1] = 0

    def weights(u, e):
        word = entries[2 * e]
        tiles = [(word >> (4 * j)) & 15 for j in range(LISTED)]
        s = stage[e]
        square = jnp.sum(jnp.where(row < 4, s * s, 0.0), axis=0, keepdims=True)
        s = jnp.where(row < 3, s, jnp.where(row == 3, square, jnp.where(row == 4, 1.0, 0.0)))
        a, b, c = three(s)
        left = jnp.concatenate([a, a, b, b, a, c], axis=0).T
        norms = [None] * 8
        for pair in range(LISTED // 2):
            rights, masses = [], []
            for j in (2 * pair, 2 * pair + 1):
                ref, base = packets[j]
                g = ref[pl.ds(base + tiles[j], 8, stride=TILES), :]
                masses.append(g[3:4])
                g = g + centred(j)
                square = jnp.sum(jnp.where(row < 3, g * g, 0.0), axis=0, keepdims=True)
                g = jnp.where(row < 3, -2.0 * g, jnp.where(row == 3, 1.0, jnp.where(row == 4, square, 0.0)))
                a, b, c = three(g)
                rights.append(jnp.concatenate([a, b, a, b, c, a], axis=0))
            q = jnp.dot(left, jnp.concatenate(rights, axis=1), preferred_element_type=jnp.float32)
            for p in range(8):
                for h in range(2):
                    part = q[16 * p : 16 * p + 16, 128 * h : 128 * h + 128]
                    k = 1.0 / (part * part)
                    mk = masses[h] * k
                    norms[p] = mk if norms[p] is None else norms[p] + mk
                    scaled = k * 65537.0
                    high = scaled - (scaled - k)
                    at = 256 * pair + 128 * h
                    split[u, 16 * p : 16 * p + 16, at : at + 128] = high
                    split[u, 128 + 16 * p : 144 + 16 * p, at : at + 128] = k - high
        norm = jnp.sum(jnp.concatenate(norms, axis=0).T, axis=0, keepdims=True)
        return tiles, norm

    def deposits(u, e, norm):
        coeff = jnp.where((lane < entries[2 * e + 1]) & (row < 5), loads[e] / norm, 0.0)
        high = coeff.astype(jnp.bfloat16).astype(jnp.float32)
        low = coeff - high
        left = jnp.concatenate(
            [jnp.concatenate([high, high], axis=1), jnp.concatenate([low, jnp.zeros_like(low)], axis=1)], axis=0
        )
        both = jnp.dot(left, split[u], preferred_element_type=jnp.float32)
        return both[0:8] + both[8:16]

    def turn(i, carry):
        done = [weights(u, TOGETHER * i + u) for u in range(TOGETHER)]
        moved = [deposits(u, TOGETHER * i + u, done[u][1]) for u in range(TOGETHER)]
        for u in range(TOGETHER):
            for j in range(LISTED):
                t = j * TILES + done[u][0][j]
                acc[t] = acc[t] + moved[u][:, 128 * j : 128 * j + 128]
        return carry

    lax.fori_loop(0, (n + TOGETHER - 1) // TOGETHER, turn, 0)
    for o in range(8):
        out = (out_0, out_y, out_x, out_xy)[o // 2]
        for q, source in enumerate((0, 2, 3, 4, 1)):
            at = o % 2 * DEP_ROWS + q * TILES
            out[at : at + TILES, :] = acc[o * TILES : (o + 1) * TILES, source, :]


def deposits_of(packets):
    vmem = pl.BlockSpec(memory_space=pltpu.VMEM)
    out = jax.ShapeDtypeStruct((2 * DEP_ROWS, 128), jnp.float32)
    return pl.pallas_call(
        deposit_kernel,
        out_shape=(out,) * 4,
        in_specs=[vmem] * 4,
        out_specs=(vmem,) * 4,
        compiler_params=pltpu.CompilerParams(vmem_limit_bytes=16 << 20),
        scratch_shapes=[
            pltpu.VMEM((16, 128), jnp.int32),
            pltpu.SMEM((16, 128), jnp.int32),
            pltpu.VMEM((CAP, 8, 128), jnp.float32),
            pltpu.VMEM((CAP, 8, 128), jnp.float32),
            pltpu.SMEM((2 * CAP,), jnp.int32),
            pltpu.VMEM((8 * TILES, 8, 128), jnp.float32),
            pltpu.VMEM((TOGETHER, 256, 1024), jnp.float32),
            pltpu.SemaphoreType.DMA,
        ],
    )(*packets)


def local(gas_pos, gas_mass, source_pos, source_radius, source_yield, source_momentum, source_tiles, source_count):
    parts = (gas_pos, gas_mass, source_pos, source_radius, source_yield, source_momentum)
    parts = [part.reshape(-1, 128) for part in parts]
    packet = packed(parts, source_tiles.reshape(BLOCKS, LISTED).T, source_count.reshape(1, 1))
    packet = jnp.concatenate([packet, shifted(packet, ("gz",), -1)], axis=0)
    sides = (("gx", "gy"), ("gy",), ("gx",))
    far = [shifted(packet, axes, -1) for axes in sides]
    own, *outward = deposits_of((packet, far[1], far[2], far[0]))
    outward = (outward[2], outward[0], outward[1])
    back = [shifted(part, axes, 1) for part, axes in zip(outward, sides)]
    total = own + back[0] + back[1] + back[2]
    total = total[:DEP_ROWS] + shifted(total[DEP_ROWS:], ("gz",), 1)
    return total.reshape(5, 1, 1, 1, TILES * 128)


def solution(mesh):
    in_specs = (
        P(None, "gx", "gy", "gz", None),
        P("gx", "gy", "gz", None),
        P(None, "gx", "gy", "gz", None),
        P("gx", "gy", "gz", None),
        P(None, "gx", "gy", "gz", None),
        P(None, "gx", "gy", "gz", None),
        P("gx", "gy", "gz", None, None),
        P("gx", "gy", "gz"),
    )
    out_specs = P(None, "gx", "gy", "gz", None)
    return jax.shard_map(local, mesh=mesh, in_specs=in_specs, out_specs=out_specs, check_vma=False)
```
